32 devices in a mesh: dp: 4 (over x, core), vocab: 8 (over z, y).
Axes of the slice: x: 2, y: 2, z: 4, core: 2. Of those that a mesh axis runs over, the one named last changes fastest.
Arguments:
- hidden: bfloat16 [512, 8192], P('dp'), may hold values from -600 to 600
- out_weight: bfloat16 [8192, 98304], P('dp', 'vocab'), may hold values from -0.5 to 0.5
- targets: int32 [512], P('dp'), may hold values from 0 to 98303
- segment: int32 [512], P('dp'), may hold values from 0 to 15, never falling along the last dimension, each value on 1 to 64 neighbouring positions
- loss_mask: int32 [512], P('dp'), may hold values 0 or 1
- outside_count: int32 [16], replicated, may hold values from 0 to 3
Outputs:
- token_loss: float32 [512], P('dp')
- sample_loss: float32 [16], replicated
The draws below stay inside these ranges and needn't reach their ends.
All inputs are finite; a program needn't handle non-finite values. No bound on the sum of `loss_mask` on one device may be relied on, other than what follows from the above.
Results may differ from the reference program's by a relative error of at most 0.0003.
Values may be sent and summed in bfloat16 or wider, within the bound.
A program may use at most 128 MiB of HBM per device.

```python
import math
import jax
import jax.numpy as jnp
import numpy as np
from jax import lax

D = 8192
V = 98304
TOKENS = 512
SAMPLES = 16
SEG_MOST = 64


def weight_full(key):
    base = jax.random.normal(jax.random.fold_in(key, 7), (D, V), jnp.float32) * D ** (-0.5)
    return base


def draw_out_weight(key, part):
    return weight_full(key).astype(jnp.bfloat16)


def draw_hidden(key, part):
    states = jax.random.normal(jax.random.fold_in(key, 21), (TOKENS, D), jnp.float32) * 3.0
    return states.astype(jnp.bfloat16)


def set_ends(entries, key, smallest, top_value):
    index_at = [jax.random.randint(jax.random.fold_in(key, axis), (), 0, length) for axis, length in enumerate(entries.shape)]
    longest = entries.shape.index(max(entries.shape))
    neighbour = index_at[:longest] + [(index_at[longest] + 1) % entries.shape[longest]] + index_at[longest + 1:]
    return entries.at[tuple(index_at)].set(smallest).at[tuple(neighbour)].set(top_value)


def ranked_wide(stream_key, shape, number_of, slope):
    portions = [min(1 << octave, number_of + 1 - (1 << octave)) * (1 << 20) // math.isqrt((1 << octave) ** slope) + 1 for octave in range((number_of + 1).bit_length()) if 1 << octave <= number_of]
    spread = 1 + sum(portions) // (1 << 30)
    grid = np.cumsum(np.array([max(1, weight // spread) for weight in portions]))
    lot = jax.random.randint(jax.random.fold_in(stream_key, 1), shape, 0, int(grid[len(portions) - 1]))
    start = jnp.left_shift(1, jnp.searchsorted(jnp.asarray(grid, jnp.int32), lot, side="right").astype(jnp.int32))
    standing = start - 1 + jax.random.randint(jax.random.fold_in(stream_key, 4), shape, 0, 1 << 30) % jnp.minimum(start, number_of + 1 - start)
    return jax.random.permutation(jax.random.fold_in(stream_key, 2), number_of)[standing].astype(jnp.int32)


def length_profile(amount, total, reach, skew):
    weights = [(1 << 20) // math.isqrt(standing ** skew) + 1 for standing in range(2, amount + 1)]
    surplus, holding = total - reach - (amount - 1), [1] * (amount - 1)
    while surplus > 0:
        candidates = [i for i in range(amount - 1) if holding[i] < reach]
        pool, left = sum([weights[i] for i in candidates]), surplus
        for i in candidates:
            extra = min(reach - holding[i], max(1, left * weights[i] // pool), surplus)
            holding[i] = holding[i] + extra
            surplus = surplus - extra
    return np.array([reach] + holding)


def uneven(rng, number_of, total, reach, skew):
    if number_of == 2:
        one = jax.random.randint(rng, (), max(1, total - reach), min(reach, total - 1) + 1)
        return jnp.stack([one, total - one])
    lengths = jnp.asarray(length_profile(number_of, total, reach, skew), jnp.int32)
    couples = (number_of - 1) // 2
    donor, receiver = lengths[1:1 + 2 * couples:2], lengths[2:2 + 2 * couples:2]
    slack = jnp.minimum(donor - 1, reach - receiver)
    moved = jax.random.randint(jax.random.fold_in(rng, 1), (couples,), 0, 1 << 20) % (slack + 1)
    lengths = lengths.at[1:1 + 2 * couples:2].set(donor - moved).at[2:2 + 2 * couples:2].set(receiver + moved)
    return lengths[jax.random.permutation(jax.random.fold_in(rng, 2), number_of)]


def setup_inputs(seed: int = 0) -> dict:
    seeds = jax.random.split(jax.random.key(seed), 7)
    return {
        "hidden": draw_hidden(jax.random.fold_in(seeds[6], 71), 0),
        "out_weight": draw_out_weight(jax.random.fold_in(seeds[6], 71), 0),
        "targets": set_ends(ranked_wide(seeds[2], (TOKENS,), V, 2), jax.random.fold_in(seeds[2], 3), 0, V - 1).astype(jnp.int32),
        "segment": jnp.searchsorted(jnp.cumsum(uneven(seeds[3], SAMPLES, TOKENS, SEG_MOST, 2)), jnp.arange(TOKENS), side="right").astype(jnp.int32),
        "loss_mask": set_ends((jax.random.randint(seeds[4], (TOKENS,), 0, 4) < 3).astype(jnp.int32), jax.random.fold_in(seeds[4], 1), 0, 1),
        "outside_count": set_ends(jax.random.randint(seeds[5], (SAMPLES,), 0, 4), jax.random.fold_in(seeds[5], 1), 0, 3).astype(jnp.int32),
    }


def reference(hidden, out_weight, targets, segment, loss_mask, outside_count):
    block_rows = math.gcd(TOKENS, 256)
    block_count = TOKENS // block_rows
    hidden_blocks = hidden.reshape(block_count, block_rows, D)
    target_blocks = targets.reshape(block_count, block_rows)

    def one_block(pair):
        rows_block, target_block = pair
        logits = jnp.dot(rows_block, out_weight, preferred_element_type=jnp.float32)
        largest = jnp.max(logits, axis=1)
        lse = largest + jnp.log(jnp.sum(jnp.exp(logits - largest[:, None]), axis=1))
        picked = jnp.take_along_axis(logits, target_block[:, None].astype(jnp.int32), axis=1)[:, 0]
        return lse - picked

    token_loss = lax.map(one_block, (hidden_blocks, target_blocks)).reshape(TOKENS)
    onehot = (segment[:, None] == jnp.arange(SAMPLES, dtype=jnp.int32)[None, :]).astype(jnp.float32)
    weights = loss_mask.astype(jnp.float32)
    loss_sum = jnp.dot(token_loss * weights, onehot, precision=lax.Precision.HIGHEST)
    count = jnp.dot(weights, onehot, precision=lax.Precision.HIGHEST)
    denom = jnp.maximum(count + outside_count.astype(jnp.float32), 1.0)
    return token_loss, loss_sum / denom
```

```python
import functools

import jax
import jax.numpy as jnp
from jax import lax
from jax.experimental import pallas as pl
from jax.experimental.pallas import tpu as pltpu
from jax.sharding import PartitionSpec as P

LANES = 128
TOP = 32767.0
TINY = 1e-30
RING = 4
WSLOTS = 4
WIDTH = 512


def largest_tile(columns, most):
    tile = most
    while columns % tile:
        tile //= 2
    return tile


def kernel(dims, hidden, weight, targets, segment, mask, outside, out,
           hx, hp, wbuf, ybuf, prt, qs, qr, ss, sr, scale_buf, tg, tcol, m_buf, s_buf, p_buf,
           info, outv, denom, stat, statr, wsem, lsem, hsem, csem_s, csem_r, fsem_s, fsem_r,
           tsem, isem, ysem, prsem, qssem, qrsem, sssem, srsem, stsem, dsem):
    dp, nv, rows, depth, tiles, tile, chunks, rounds = dims
    chips = dp // 2
    me, v = lax.axis_index("dp"), lax.axis_index("vocab")
    x, c = me // 2, me % 2
    partner = 2 * x + (1 - c)
    owner = 2 * lax.rem(x + 1, chips) + c
    source = 2 * lax.rem(x + chips - 1, chips) + c
    share = rows // chunks
    total_steps = chips * tiles

    def remote(src, dst, send, recv, d, w):
        return pltpu.make_async_remote_copy(
            src_ref=src, dst_ref=dst, send_sem=send, recv_sem=recv,
            device_id=(d, w), device_id_type=pl.DeviceIdType.MESH)

    def wcopy(t, slot):
        return pltpu.make_async_copy(
            weight.at[:, pl.ds(pl.multiple_of(t * tile, tile), tile)], wbuf.at[slot], wsem.at[slot])

    def features(d):
        return pl.ds(pl.multiple_of(d * depth, depth), depth)

    def token_rows(d):
        return pl.ds(pl.multiple_of(d * rows, rows), rows)

    def chunk_rows(d, j):
        return pl.ds(pl.multiple_of(d * rows + j * share, share), share)

    barrier = pltpu.get_barrier_semaphore()

    def signal(sem, d, w):
        pl.semaphore_signal(sem, inc=1, device_id=(d, w), device_id_type=pl.DeviceIdType.MESH)

    for o in range(1, dp):
        signal(barrier, lax.rem(me + o, dp), v)
    pl.when(v >= 1)(lambda: signal(barrier, me, v - 1))
    pl.when(v < nv - 1)(lambda: signal(barrier, me, v + 1))

    to_stage = pltpu.make_async_copy(hidden.at[:, features(partner)], hp, lsem.at[0])
    to_stage.start()
    own = pltpu.make_async_copy(hidden.at[:, features(me)], hx.at[token_rows(me)], lsem.at[1])
    own.start()
    for k in range(min(WSLOTS - 1, total_steps)):
        wcopy(k % tiles, k).start()

    def sides(reach):
        return jnp.where(v >= reach, 1, 0) + jnp.where(v < nv - reach, 1, 0)

    pl.semaphore_wait(barrier, dp - 1 + sides(1))

    def tell(k):
        reach = 1 << k
        pl.when(v >= reach)(lambda: signal(dsem.at[k], me, v - reach))
        pl.when(v < nv - reach)(lambda: signal(dsem.at[k], me, v + reach))

    def hear(k):
        pl.semaphore_wait(dsem.at[k], sides(1 << k))

    to_partner = remote(hp, hx.at[token_rows(me)], hsem.at[0], hsem.at[1], partner, v)
    targets_copy = remote(targets, tg, tsem.at[0], tsem.at[1], source, v)

    def crossing(step, e):
        d = 2 * lax.rem(x + step, chips) + e
        src = hidden.at[pl.ds(pl.multiple_of(v * share, share), share), features(d)]
        i = 2 * (step - 1) + e
        r = 2 * (chips - step - 1) + c
        return d, src, i, r

    def cross_start():
        for step in range(1, chips):
            for e in range(2):
                d, src, i, r = crossing(step, e)
                remote(src, hx.at[chunk_rows(me, v)], csem_s.at[i], csem_r.at[r], d, v).start()

    def if_sender(fn):
        if chunks < nv:
            pl.when(v < chunks)(fn)
        else:
            fn()

    if_sender(cross_start)
    if rounds:
        tell(0)
    to_stage.wait()
    to_partner.start()

    local_info = [pltpu.make_async_copy(ref, info.at[me, k], lsem.at[2])
                  for k, ref in enumerate((segment, mask))]
    local_out = pltpu.make_async_copy(outside, outv, lsem.at[3])

    def info_copy(o, k, ref):
        return remote(ref, info.at[me, k], isem.at[0], isem.at[1], lax.rem(me + o, dp), v)

    def start_small():
        targets_copy.start()
        for o in range(1, dp):
            for k, ref in enumerate((segment, mask)):
                info_copy(o, k, ref).start()
        for copy in local_info:
            copy.start()
        local_out.start()

    def spread():
        for step in range(1, chips):
            for e in range(2):
                d = 2 * lax.rem(x + step, chips) + e
                i = 2 * (step - 1) + e
                block = hx.at[chunk_rows(d, v)]
                remote(block, block, csem_s.at[i], csem_r.at[i], d, v).wait_recv()

                def one(o, carry, block=block, step=step, i=i):
                    w = lax.rem(v + o, nv)
                    remote(block, block, fsem_s.at[i], fsem_r.at[step - 1], me, w).start()
                    return carry

                lax.fori_loop(1, nv, one, 0)

    def blocks_wait(count, sem_s, sem_r, send):
        block = hx.at[pl.ds(0, count)]
        copy = remote(block, block, sem_s, sem_r, partner, v)
        if send:
            copy.wait_send()
        else:
            copy.wait_recv()

    def spread_wait(step):
        if chunks < nv:
            pl.when(v < chunks)(lambda: blocks_wait(
                2 * (chunks - 1) * share, fsem_s.at[0], fsem_r.at[step - 1], False))
            pl.when(v >= chunks)(lambda: blocks_wait(
                2 * chunks * share, fsem_s.at[0], fsem_r.at[step - 1], False))
        else:
            blocks_wait(2 * (chunks - 1) * share, fsem_s.at[0], fsem_r.at[step - 1], False)

    def dot_rows(start, count, at, slot, yslot):
        lhs = pl.ds(pl.multiple_of(start, count), count)
        ybuf[yslot, pl.ds(pl.multiple_of(at, count), count), :] = jnp.dot(
            hx[lhs, :], wbuf[slot], preferred_element_type=jnp.float32)

    def ycopy(i):
        half = pl.ds(pl.multiple_of((1 - c) * rows, rows), rows)
        slot, ring = lax.rem(i, 2), lax.rem(i, RING)
        return remote(ybuf.at[slot, half], prt.at[ring], ysem.at[slot], prsem.at[ring], partner, v)

    def qcopy(s, t):
        d = 2 * lax.rem(x + chips - s - 1 + chips, chips) + c
        return (remote(qs.at[s, t], qr.at[s, t], qssem, qrsem.at[s, t], d, v),
                remote(ss.at[s, t], sr.at[s, t], sssem, srsem.at[s, t], d, v))

    band = min(rows, 32)

    def total(i, b):
        mine = pl.ds(pl.multiple_of(c * rows + b * band, band), band)
        theirs = pl.ds(b * band, band)
        return ybuf[lax.rem(i, 2), mine, :] + prt[lax.rem(i, RING), theirs, :]

    def send_sums(s, t):
        i = s * tiles + t
        ycopy(i).wait_recv()
        for b in range(rows // band):
            value = total(i, b)
            top = jnp.maximum(jnp.max(jnp.abs(value), axis=1, keepdims=True), TINY)
            code = jnp.round(value * (TOP / top)).astype(jnp.int32)
            qs[s, t, b * band:(b + 1) * band, :] = code.astype(jnp.int16)
            scale_buf[b * band:(b + 1) * band, :] = jnp.broadcast_to(top * (1.0 / TOP), (band, LANES))
        data, scales = qcopy(s, t)
        data.start()
        ss[s, t] = jnp.transpose(scale_buf[0:rows, :])[0:1, :]
        scales.start()

    def finish(s, t):
        i = s * tiles + t
        ycopy(i).wait_recv()
        for a in range(chips - 1):
            for copy in qcopy(a, t):
                copy.wait_recv()
            scale_buf[a * rows:(a + 1) * rows, :] = jnp.transpose(
                jnp.broadcast_to(sr[a, t], (LANES, rows)))
        base = v * (tiles * tile) + t * tile
        lane = lax.broadcasted_iota(jnp.int32, (band, LANES), 1)
        for b in range(rows // band):
            here = slice(b * band, (b + 1) * band)
            value = total(i, b)
            parts = []
            for k in range(tile // LANES):
                part = value[:, k * LANES:(k + 1) * LANES]
                for a in range(chips - 1):
                    code = qr[a, t, here, k * LANES:(k + 1) * LANES].astype(jnp.int32)
                    part = part + code.astype(jnp.float32) * scale_buf[a * rows + b * band:a * rows + (b + 1) * band, :]
                parts.append(part)
            old = m_buf[here, :]
            new = functools.reduce(jnp.maximum, parts, old)
            acc = s_buf[here, :] * jnp.exp(old - new)
            picked = p_buf[here, :]
            wanted = tcol[here, :] - base
            for k, part in enumerate(parts):
                acc = acc + jnp.exp(part - new)
                picked = picked + jnp.where(lane + k * LANES == wanted, part, 0.0)
            m_buf[here, :] = new
            s_buf[here, :] = acc
            p_buf[here, :] = picked

    m_buf[...] = jnp.full(m_buf.shape, -jnp.inf, jnp.float32)
    s_buf[...] = jnp.zeros(s_buf.shape, jnp.float32)
    p_buf[...] = jnp.zeros(p_buf.shape, jnp.float32)
    own.wait()

    events = []
    events.append((1, start_small))
    for k in range(rounds):
        def turn(k=k):
            hear(k)
            if k + 1 < rounds:
                tell(k + 1)
        events.append((2 + 2 * k, turn))
    events.append((2 + 2 * rounds, lambda: if_sender(spread)))

    samples = outside.shape[1]

    def prepare():
        targets_copy.wait_recv()
        tcol[...] = jnp.transpose(jnp.broadcast_to(tg[...], (LANES, rows)))
        most = info.at[pl.ds(0, dp - 1)]
        remote(most, most, isem.at[0], isem.at[1], partner, v).wait_recv()
        pltpu.make_async_copy(info.at[me], info.at[me], lsem.at[2]).wait()
        local_out.wait()
        count = jnp.zeros((samples, 1), jnp.float32)
        for d in range(dp):
            member = lax.broadcasted_iota(jnp.int32, (samples, rows), 0) == info[d, 0]
            weights = info[d, 1].astype(jnp.float32)
            count = count + jnp.sum(jnp.where(member, weights, 0.0), axis=1, keepdims=True)
        square = (lax.broadcasted_iota(jnp.int32, (samples, samples), 0)
                  == lax.broadcasted_iota(jnp.int32, (samples, samples), 1))
        away = jnp.sum(jnp.where(square, outv[...].astype(jnp.float32), 0.0), axis=1, keepdims=True)
        denom[...] = jnp.broadcast_to(jnp.maximum(count + away, 1.0), (samples, LANES))

    for s in range(chips):
        group = lax.rem(x + chips - s, chips)
        last = s == chips - 1
        if s > 0:
            spread_wait(chips - s)
        if last:
            prepare()
        handle = finish if last else send_sums

        def begin(i):
            slot = lax.rem(i, WSLOTS)
            wcopy(lax.rem(i, tiles), slot).wait()

            @pl.when(i + WSLOTS - 1 < total_steps)
            def _():
                wcopy(lax.rem(i + WSLOTS - 1, tiles), lax.rem(i + WSLOTS - 1, WSLOTS)).start()

            return slot

        def step(t, carry, s=s, group=group, handle=handle, begin=begin):
            i = s * tiles + t
            slot = begin(i)

            @pl.when(i >= 2)
            def _():
                ycopy(i).wait_send()

            dot_rows(group * 2 * rows, 2 * rows, 0, slot, lax.rem(i, 2))
            ycopy(i).start()

            @pl.when(t >= 1)
            def _():
                handle(s, t - 1)

            if s == 0:
                for at, event in events:
                    pl.when(t == min(at, tiles - 1))(event)
            return carry

        first = 0
        if s == 0:
            slot = begin(0)
            dot_rows(me * rows, rows, c * rows, slot, 0)
            to_partner.wait_recv()
            dot_rows(partner * rows, rows, (1 - c) * rows, slot, 0)
            ycopy(0).start()
            for at, event in events:
                if min(at, tiles - 1) == 0:
                    event()
            first = 1
        lax.fori_loop(first, tiles, step, 0)
        handle(s, tiles - 1)

    lane = lax.broadcasted_iota(jnp.int32, (rows, LANES), 1)
    peak = jnp.max(m_buf[...], axis=1, keepdims=True)
    mass = jnp.sum(s_buf[...] * jnp.exp(m_buf[...] - peak), axis=1, keepdims=True)
    hit = jnp.sum(p_buf[...], axis=1, keepdims=True)
    table = jnp.transpose(jnp.where(lane == 0, peak, jnp.where(lane == 1, mass, hit)))
    stat[0:1, :] = table[0:1, :] + jnp.log(table[1:2, :])
    stat[1:2, :] = table[2:3, :]

    def stat_copy(d, w):
        return remote(stat, statr.at[owner * nv + v], stsem.at[0], stsem.at[1], d, w)

    def stat_start(o, carry):
        w = lax.rem(v + o, nv)
        for k in range(dp):
            stat_copy(lax.rem(me + k, dp), w).start()
        return carry

    lax.fori_loop(1, nv, stat_start, 0)
    for k in range(1, dp):
        stat_copy(lax.rem(me + k, dp), v).start()
    statr[owner * nv + v] = stat[...]
    most = statr.at[pl.ds(0, dp * nv - 1)]
    remote(most, most, stsem.at[0], stsem.at[1], partner, v).wait_recv()

    mine = jnp.zeros((1, rows), jnp.float32)
    sums = jnp.zeros((samples, rows), jnp.float32)
    for d in range(dp):
        block = statr[d * nv:(d + 1) * nv]
        peak = jnp.max(block, axis=0)
        mass = jnp.sum(jnp.exp(block - peak[None]), axis=0)
        hit = jnp.sum(block, axis=0)
        loss = peak[0:1, :] + jnp.log(mass[0:1, :]) - hit[1:2, :]
        mine = jnp.where(me == d, loss, mine)
        member = lax.broadcasted_iota(jnp.int32, (samples, rows), 0) == info[d, 0]
        sums = sums + jnp.where(member, loss * info[d, 1].astype(jnp.float32), 0.0)
    ratio = jnp.sum(sums, axis=1, keepdims=True) / denom[:, 0:1]
    wide = out.shape[1] - rows
    diagonal = (lax.broadcasted_iota(jnp.int32, (samples, wide), 0)
                == lax.broadcasted_iota(jnp.int32, (samples, wide), 1))
    out[0:1, 0:rows] = mine
    out[0:1, rows:rows + wide] = jnp.sum(jnp.where(diagonal, ratio, 0.0), axis=0, keepdims=True)

    to_partner.wait_send()
    targets_copy.wait_send()
    most_info = info.at[pl.ds(0, dp - 1)]
    remote(most_info, most_info, isem.at[0], isem.at[1], partner, v).wait_send()

    def leave():
        for step in range(1, chips):
            for e in range(2):
                d, src, i, r = crossing(step, e)
                remote(src, hx.at[chunk_rows(me, v)], csem_s.at[i], csem_r.at[r], d, v).wait_send()
        for step in range(1, chips):
            for e in range(2):
                i = 2 * (step - 1) + e
                blocks_wait((nv - 1) * share, fsem_s.at[i], fsem_r.at[step - 1], True)

    if_sender(leave)
    for k in range(min(2, total_steps)):
        ycopy(k).wait_send()
    remote(qs, qr, qssem, qrsem.at[0, 0], partner, v).wait_send()
    remote(ss, sr, sssem, srsem.at[0, 0], partner, v).wait_send()
    remote(most, most, stsem.at[0], stsem.at[1], partner, v).wait_send()


def solution(mesh):
    dp, nv = mesh.shape["dp"], mesh.shape["vocab"]

    def body(hidden, out_weight, targets, segment, loss_mask, outside_count):
        rows = hidden.shape[0]
        depth, columns = out_weight.shape
        samples = outside_count.shape[0]
        chips = dp // 2
        tile = largest_tile(columns, WIDTH)
        tiles = columns // tile
        chunks = min(nv, rows // 16)
        rounds = (nv - 2).bit_length()
        dims = (dp, nv, rows, depth, tiles, tile, chunks, rounds)
        sem = pltpu.SemaphoreType.DMA
        far = 2 * (chips - 1)
        wide = -(-samples // LANES) * LANES
        vm = pl.BlockSpec(memory_space=pltpu.VMEM)
        hbm = pl.BlockSpec(memory_space=pl.ANY)
        res = pl.pallas_call(
            functools.partial(kernel, dims),
            out_shape=jax.ShapeDtypeStruct((1, rows + wide), jnp.float32),
            in_specs=[hbm] * 6,
            out_specs=vm,
            scratch_shapes=[
                pltpu.VMEM((dp * rows, depth), jnp.bfloat16),
                pltpu.VMEM((rows, depth), jnp.bfloat16),
                pltpu.VMEM((WSLOTS, depth, tile), jnp.bfloat16),
                pltpu.VMEM((2, 2 * rows, tile), jnp.float32),
                pltpu.VMEM((RING, rows, tile), jnp.float32),
                pltpu.VMEM((chips - 1, tiles, rows, tile), jnp.int16),
                pltpu.VMEM((chips - 1, tiles, rows, tile), jnp.int16),
                pltpu.VMEM((chips - 1, tiles, 1, rows), jnp.float32),
                pltpu.VMEM((chips - 1, tiles, 1, rows), jnp.float32),
                pltpu.VMEM(((chips - 1) * rows, LANES), jnp.float32),
                pltpu.VMEM((1, rows), jnp.int32),
                pltpu.VMEM((rows, LANES), jnp.int32),
                pltpu.VMEM((rows, LANES), jnp.float32),
                pltpu.VMEM((rows, LANES), jnp.float32),
                pltpu.VMEM((rows, LANES), jnp.float32),
                pltpu.VMEM((dp, 2, 1, rows), jnp.int32),
                pltpu.VMEM((1, samples), jnp.int32),
                pltpu.VMEM((samples, LANES), jnp.float32),
                pltpu.VMEM((2, rows), jnp.float32),
                pltpu.VMEM((dp * nv, 2, rows), jnp.float32),
                sem((WSLOTS,)), sem((4,)), sem((2,)), sem((far,)), sem((far,)),
                sem((far,)), sem((chips - 1,)), sem((2,)), sem((2,)),
                sem((2,)), sem((RING,)),
                sem, sem((chips - 1, tiles)), sem, sem((chips - 1, tiles)),
                sem((2,)), pltpu.SemaphoreType.REGULAR((max(rounds, 1),)),
            ],
            compiler_params=pltpu.CompilerParams(
                collective_id=0, has_side_effects=True, vmem_limit_bytes=60 * 1024 * 1024),
        )(hidden, out_weight, targets[None, :], segment[None, :], loss_mask[None, :],
          outside_count[None, :])
        return res[0, :rows], res[0, rows:rows + samples]

    return jax.shard_map(
        body,
        mesh=mesh,
        in_specs=(P("dp", None), P("dp", "vocab"), P("dp"), P("dp"), P("dp"), P()),
        out_specs=(P("dp"), P()),
        check_vma=False,
    )
```

```python
import functools

import jax
import jax.numpy as jnp
from jax import lax
from jax.experimental import pallas as pl
from jax.experimental.pallas import tpu as pltpu
from jax.sharding import PartitionSpec as P

LANES = 128
TOP = 32767.0
TINY = 1e-30
RING = 4
WSLOTS = 4
WIDTH = 512
HEAD = 128


def largest_tile(columns, most):
    tile = most
    while columns % tile:
        tile //= 2
    return tile


def kernel(dims, hidden, weight, targets, segment, mask, outside, out,
           hx, hp, cx, wbuf, ybuf, prt, qs, qr, ss, sr, scale_buf, tg, tcol, m_buf, s_buf, p_buf,
           info, outv, denom, stat, statr, wsem, wfirst, lsem, hsem, csem_s, csem_r, fsem_s, fsem_r,
           tsem, isem, ysem, prsem, prfirst, qssem, qrsem, sssem, srsem, stsem, dsem):
    dp, nv, rows, depth, tiles, tile, chunks, rounds, heads = dims
    chips = dp // 2
    me, v = lax.axis_index("dp"), lax.axis_index("vocab")
    x, c = me // 2, me % 2
    partner = 2 * x + (1 - c)
    owner = 2 * lax.rem(x + 1, chips) + c
    source = 2 * lax.rem(x + chips - 1, chips) + c
    share = rows // chunks
    total_steps = chips * tiles
    extra = len(heads) - 1

    def remote(src, dst, send, recv, d, w):
        return pltpu.make_async_remote_copy(
            src_ref=src, dst_ref=dst, send_sem=send, recv_sem=recv,
            device_id=(d, w), device_id_type=pl.DeviceIdType.MESH)

    def wcopy(t, slot):
        return pltpu.make_async_copy(
            weight.at[:, pl.ds(pl.multiple_of(t * tile, tile), tile)], wbuf.at[slot], wsem.at[slot])

    def features(d):
        return pl.ds(pl.multiple_of(d * depth, depth), depth)

    def token_rows(d):
        return pl.ds(pl.multiple_of(d * rows, rows), rows)

    def chunk_rows(d, j):
        return pl.ds(pl.multiple_of(d * rows + j * share, share), share)

    def crossing(step, e):
        d = 2 * lax.rem(x + step, chips) + e
        return d, 2 * (step - 1) + e, 2 * (chips - step - 1) + c

    def cross_start():
        pltpu.make_async_copy(cx, cx, lsem.at[4]).wait()
        for step in range(1, chips):
            for e in range(2):
                d, i, r = crossing(step, e)
                remote(cx.at[i], hx.at[chunk_rows(me, v)], csem_s.at[i], csem_r.at[r], d, v).start()

    def if_sender(fn):
        if chunks < nv:
            pl.when(v < chunks)(fn)
        else:
            fn()

    barrier = pltpu.get_barrier_semaphore()

    def signal(sem, d, w):
        pl.semaphore_signal(sem, inc=1, device_id=(d, w), device_id_type=pl.DeviceIdType.MESH)

    for o in range(1, dp):
        signal(barrier, lax.rem(me + o, dp), v)
    pl.when(v >= 1)(lambda: signal(barrier, me, v - 1))
    pl.when(v < nv - 1)(lambda: signal(barrier, me, v + 1))

    to_stage = pltpu.make_async_copy(hidden.at[:, features(partner)], hp, lsem.at[0])
    to_stage.start()

    def cross_load():
        for step in range(1, chips):
            for e in range(2):
                d, i, r = crossing(step, e)
                src = hidden.at[pl.ds(pl.multiple_of(v * share, share), share), features(d)]
                pltpu.make_async_copy(src, cx.at[i], lsem.at[4]).start()

    if_sender(cross_load)
    own = pltpu.make_async_copy(hidden.at[:, features(me)], hx.at[token_rows(me)], lsem.at[1])
    own.start()

    def first_copy(k):
        cols = pl.ds(*heads[k])
        return pltpu.make_async_copy(weight.at[:, cols], wbuf.at[0, :, cols], wfirst.at[k])

    for k in range(len(heads)):
        first_copy(k).start()

    def sides(reach):
        return jnp.where(v >= reach, 1, 0) + jnp.where(v < nv - reach, 1, 0)

    pl.semaphore_wait(barrier, dp - 1 + sides(1))

    def tell(k):
        reach = 1 << k
        pl.when(v >= reach)(lambda: signal(dsem.at[k], me, v - reach))
        pl.when(v < nv - reach)(lambda: signal(dsem.at[k], me, v + reach))

    def hear(k):
        pl.semaphore_wait(dsem.at[k], sides(1 << k))

    to_partner = remote(hp, hx.at[token_rows(me)], hsem.at[0], hsem.at[1], partner, v)
    targets_copy = remote(targets, tg, tsem.at[0], tsem.at[1], source, v)

    to_stage.wait()
    to_partner.start()
    if_sender(cross_start)
    if rounds:
        tell(0)
    for k in range(1, min(WSLOTS, total_steps)):
        wcopy(k % tiles, k).start()

    local_info = [pltpu.make_async_copy(ref, info.at[me, k], lsem.at[2])
                  for k, ref in enumerate((segment, mask))]
    local_out = pltpu.make_async_copy(outside, outv, lsem.at[3])

    def info_copy(o, k, ref):
        return remote(ref, info.at[me, k], isem.at[0], isem.at[1], lax.rem(me + o, dp), v)

    def start_small():
        targets_copy.start()
        for o in range(1, dp):
            for k, ref in enumerate((segment, mask)):
                info_copy(o, k, ref).start()
        for copy in local_info:
            copy.start()
        local_out.start()

    def spread():
        for step in range(1, chips):
            for e in range(2):
                d = 2 * lax.rem(x + step, chips) + e
                i = 2 * (step - 1) + e
                block = hx.at[chunk_rows(d, v)]
                remote(block, block, csem_s.at[i], csem_r.at[i], d, v).wait_recv()

                def one(o, carry, block=block, step=step, i=i):
                    w = lax.rem(v + o, nv)
                    remote(block, block, fsem_s.at[i], fsem_r.at[step - 1], me, w).start()
                    return carry

                lax.fori_loop(1, nv, one, 0)

    def blocks_wait(count, sem_s, sem_r, send):
        block = hx.at[pl.ds(0, count)]
        copy = remote(block, block, sem_s, sem_r, partner, v)
        if send:
            copy.wait_send()
        else:
            copy.wait_recv()

    def spread_wait(step):
        if chunks < nv:
            pl.when(v < chunks)(lambda: blocks_wait(
                2 * (chunks - 1) * share, fsem_s.at[0], fsem_r.at[step - 1], False))
            pl.when(v >= chunks)(lambda: blocks_wait(
                2 * chunks * share, fsem_s.at[0], fsem_r.at[step - 1], False))
        else:
            blocks_wait(2 * (chunks - 1) * share, fsem_s.at[0], fsem_r.at[step - 1], False)

    def dot_rows(start, count, at, slot, yslot, first=0, width=tile):
        lhs = pl.ds(pl.multiple_of(start, count), count)
        cols = slice(first, first + width)
        ybuf[yslot, pl.ds(pl.multiple_of(at, count), count), cols] = jnp.dot(
            hx[lhs, :], wbuf[slot, :, cols], preferred_element_type=jnp.float32)

    def ycopy(i):
        half = pl.ds(pl.multiple_of((1 - c) * rows, rows), rows)
        slot, ring = lax.rem(i, 2), lax.rem(i, RING)
        return remote(ybuf.at[slot, half], prt.at[ring], ysem.at[slot], prsem.at[ring], partner, v)

    def first_ycopy(k):
        half = pl.ds(pl.multiple_of((1 - c) * rows, rows), rows)
        cols = pl.ds(*heads[k])
        return remote(ybuf.at[0, half, cols], prt.at[0, :, cols], ysem.at[0], prfirst.at[k], partner, v)

    def qcopy(s, t, k, first, width):
        d = 2 * lax.rem(x + chips - s - 1 + chips, chips) + c
        cols = pl.ds(first, width)
        return (remote(qs.at[s, t, :, cols], qr.at[s, t, :, cols], qssem, qrsem.at[s, k], d, v),
                remote(ss.at[s, k], sr.at[s, k], sssem, srsem.at[s, k], d, v))

    band = min(rows, 32)

    def total(i, b, cols):
        mine = pl.ds(pl.multiple_of(c * rows + b * band, band), band)
        theirs = pl.ds(b * band, band)
        return ybuf[lax.rem(i, 2), mine, cols] + prt[lax.rem(i, RING), theirs, cols]

    def send_sums(s, t, k, first, width):
        i = s * tiles + t
        cols = slice(first, first + width)
        for b in range(rows // band):
            value = total(i, b, cols)
            top = jnp.maximum(jnp.max(jnp.abs(value), axis=1, keepdims=True), TINY)
            code = jnp.round(value * (TOP / top)).astype(jnp.int32)
            qs[s, t, b * band:(b + 1) * band, cols] = code.astype(jnp.int16)
            scale_buf[b * band:(b + 1) * band, :] = jnp.broadcast_to(top * (1.0 / TOP), (band, LANES))
        data, scales = qcopy(s, t, k, first, width)
        data.start()
        ss[s, k] = jnp.transpose(scale_buf[0:rows, :])[0:1, :]
        scales.start()

    def finish(s, t, k, first, width):
        i = s * tiles + t
        for a in range(chips - 1):
            for copy in qcopy(a, t, k, first, width):
                copy.wait_recv()
            scale_buf[a * rows:(a + 1) * rows, :] = jnp.transpose(
                jnp.broadcast_to(sr[a, k], (LANES, rows)))
        base = v * (tiles * tile) + t * tile + first
        lane = lax.broadcasted_iota(jnp.int32, (band, LANES), 1)
        for b in range(rows // band):
            here = slice(b * band, (b + 1) * band)
            value = total(i, b, slice(first, first + width))
            parts = []
            for j in range(width // LANES):
                part = value[:, j * LANES:(j + 1) * LANES]
                from_here = slice(first + j * LANES, first + (j + 1) * LANES)
                for a in range(chips - 1):
                    code = qr[a, t, here, from_here].astype(jnp.int32)
                    part = part + code.astype(jnp.float32) * scale_buf[a * rows + b * band:a * rows + (b + 1) * band, :]
                parts.append(part)
            old = m_buf[here, :]
            new = functools.reduce(jnp.maximum, parts, old)
            acc = s_buf[here, :] * jnp.exp(old - new)
            picked = p_buf[here, :]
            wanted = tcol[here, :] - base
            for j, part in enumerate(parts):
                acc = acc + jnp.exp(part - new)
                picked = picked + jnp.where(lane + j * LANES == wanted, part, 0.0)
            m_buf[here, :] = new
            s_buf[here, :] = acc
            p_buf[here, :] = picked

    m_buf[...] = jnp.full(m_buf.shape, -jnp.inf, jnp.float32)
    s_buf[...] = jnp.zeros(s_buf.shape, jnp.float32)
    p_buf[...] = jnp.zeros(p_buf.shape, jnp.float32)
    own.wait()

    events = []
    events.append((1, start_small))
    for k in range(rounds):
        def turn(k=k):
            hear(k)
            if k + 1 < rounds:
                tell(k + 1)
        events.append((2 + 2 * k, turn))
    events.append((2 + 2 * rounds, lambda: if_sender(spread)))

    samples = outside.shape[1]

    def prepare():
        targets_copy.wait_recv()
        tcol[...] = jnp.transpose(jnp.broadcast_to(tg[...], (LANES, rows)))
        most = info.at[pl.ds(0, dp - 1)]
        remote(most, most, isem.at[0], isem.at[1], partner, v).wait_recv()
        pltpu.make_async_copy(info.at[me], info.at[me], lsem.at[2]).wait()
        local_out.wait()
        count = jnp.zeros((samples, 1), jnp.float32)
        for d in range(dp):
            member = lax.broadcasted_iota(jnp.int32, (samples, rows), 0) == info[d, 0]
            weights = info[d, 1].astype(jnp.float32)
            count = count + jnp.sum(jnp.where(member, weights, 0.0), axis=1, keepdims=True)
        square = (lax.broadcasted_iota(jnp.int32, (samples, samples), 0)
                  == lax.broadcasted_iota(jnp.int32, (samples, samples), 1))
        away = jnp.sum(jnp.where(square, outv[...].astype(jnp.float32), 0.0), axis=1, keepdims=True)
        denom[...] = jnp.broadcast_to(jnp.maximum(count + away, 1.0), (samples, LANES))

    for s in range(chips):
        group = lax.rem(x + chips - s, chips)
        last = s == chips - 1
        if s > 0:
            spread_wait(chips - s)
        if last:
            prepare()
        piece = finish if last else send_sums

        def handle(t, s=s, piece=piece):
            ycopy(s * tiles + t).wait_recv()
            piece(s, t, t + extra, 0, tile)

        def begin(i):
            slot = lax.rem(i, WSLOTS)
            wcopy(lax.rem(i, tiles), slot).wait()

            @pl.when(i + WSLOTS - 1 < total_steps)
            def _():
                wcopy(lax.rem(i + WSLOTS - 1, tiles), lax.rem(i + WSLOTS - 1, WSLOTS)).start()

            return slot

        def step(t, carry, s=s, group=group, handle=handle, begin=begin):
            i = s * tiles + t
            slot = begin(i)

            @pl.when(i >= 2)
            def _():
                ycopy(i).wait_send()

            dot_rows(group * 2 * rows, 2 * rows, 0, slot, lax.rem(i, 2))
            ycopy(i).start()

            @pl.when(t >= 2)
            def _():
                handle(t - 1)

            if s == 0:
                for at, event in events:
                    pl.when(t == min(at, tiles - 1))(event)
            return carry

        if s == 0:
            for k in range(len(heads)):
                first_copy(k).wait()
                dot_rows(me * rows, rows, c * rows, 0, 0, *heads[k])
            to_partner.wait_recv()
            for k in range(len(heads)):
                dot_rows(partner * rows, rows, (1 - c) * rows, 0, 0, *heads[k])
                first_ycopy(k).start()
            for k in range(len(heads)):
                first_ycopy(k).wait_recv()
                piece(s, 0, k, *heads[k])
            if tiles == 1:
                for at, event in events:
                    event()
        else:
            i = s * tiles
            slot = begin(i)
            if i >= 2:
                ycopy(i).wait_send()
            dot_rows(group * 2 * rows, 2 * rows, 0, slot, i % 2)
            ycopy(i).start()
            ycopy(i).wait_recv()
            for k in range(len(heads)):
                piece(s, 0, k, *heads[k])
        if tiles > 1:
            lax.fori_loop(1, tiles, step, 0)
            handle(tiles - 1)

    lane = lax.broadcasted_iota(jnp.int32, (rows, LANES), 1)
    peak = jnp.max(m_buf[...], axis=1, keepdims=True)
    mass = jnp.sum(s_buf[...] * jnp.exp(m_buf[...] - peak), axis=1, keepdims=True)
    hit = jnp.sum(p_buf[...], axis=1, keepdims=True)
    table = jnp.transpose(jnp.where(lane == 0, peak, jnp.where(lane == 1, mass, hit)))
    stat[0:1, :] = table[0:1, :] + jnp.log(table[1:2, :])
    stat[1:2, :] = table[2:3, :]

    def stat_copy(d, w):
        return remote(stat, statr.at[owner * nv + v], stsem.at[0], stsem.at[1], d, w)

    def stat_start(o, carry):
        w = lax.rem(v + o, nv)
        for k in range(dp):
            stat_copy(lax.rem(me + k, dp), w).start()
        return carry

    lax.fori_loop(1, nv, stat_start, 0)
    for k in range(1, dp):
        stat_copy(lax.rem(me + k, dp), v).start()
    statr[owner * nv + v] = stat[...]
    most = statr.at[pl.ds(0, dp * nv - 1)]
    remote(most, most, stsem.at[0], stsem.at[1], partner, v).wait_recv()

    mine = jnp.zeros((1, rows), jnp.float32)
    sums = jnp.zeros((samples, rows), jnp.float32)
    for d in range(dp):
        block = statr[d * nv:(d + 1) * nv]
        peak = jnp.max(block, axis=0)
        mass = jnp.sum(jnp.exp(block - peak[None]), axis=0)
        hit = jnp.sum(block, axis=0)
        loss = peak[0:1, :] + jnp.log(mass[0:1, :]) - hit[1:2, :]
        mine = jnp.where(me == d, loss, mine)
        member = lax.broadcasted_iota(jnp.int32, (samples, rows), 0) == info[d, 0]
        sums = sums + jnp.where(member, loss * info[d, 1].astype(jnp.float32), 0.0)
    ratio = jnp.sum(sums, axis=1, keepdims=True) / denom[:, 0:1]
    wide = out.shape[1] - rows
    diagonal = (lax.broadcasted_iota(jnp.int32, (samples, wide), 0)
                == lax.broadcasted_iota(jnp.int32, (samples, wide), 1))
    out[0:1, 0:rows] = mine
    out[0:1, rows:rows + wide] = jnp.sum(jnp.where(diagonal, ratio, 0.0), axis=0, keepdims=True)

    to_partner.wait_send()
    targets_copy.wait_send()
    most_info = info.at[pl.ds(0, dp - 1)]
    remote(most_info, most_info, isem.at[0], isem.at[1], partner, v).wait_send()

    def leave():
        for step in range(1, chips):
            for e in range(2):
                d, i, r = crossing(step, e)
                remote(cx.at[i], hx.at[chunk_rows(me, v)], csem_s.at[i], csem_r.at[r], d, v).wait_send()
        for step in range(1, chips):
            for e in range(2):
                i = 2 * (step - 1) + e
                blocks_wait((nv - 1) * share, fsem_s.at[i], fsem_r.at[step - 1], True)

    if_sender(leave)
    for k in range(min(2, total_steps)):
        ycopy(k).wait_send()
    remote(qs, qr, qssem, qrsem.at[0, 0], partner, v).wait_send()
    remote(ss, sr, sssem, srsem.at[0, 0], partner, v).wait_send()
    remote(most, most, stsem.at[0], stsem.at[1], partner, v).wait_send()


def split(res, loss, sample):
    rows, samples = loss.shape[1], sample.shape[1]
    loss[...] = res[:, 0:rows]
    sample[...] = res[:, rows:rows + samples]


def solution(mesh):
    dp, nv = mesh.shape["dp"], mesh.shape["vocab"]

    def body(hidden, out_weight, targets, segment, loss_mask, outside_count):
        rows = hidden.shape[0]
        depth, columns = out_weight.shape
        samples = outside_count.shape[0]
        chips = dp // 2
        tile = largest_tile(columns, WIDTH)
        tiles = columns // tile
        chunks = min(nv, rows // 16)
        share = rows // chunks
        rounds = (nv - 2).bit_length()
        heads, at = [], 0
        while at < tile:
            width = HEAD if at < 2 * HEAD and tile > HEAD else tile - at
            heads.append((at, width))
            at += width
        pieces = tiles + len(heads) - 1
        dims = (dp, nv, rows, depth, tiles, tile, chunks, rounds, tuple(heads))
        sem = pltpu.SemaphoreType.DMA
        far = 2 * (chips - 1)
        wide = -(-samples // LANES) * LANES
        vm = pl.BlockSpec(memory_space=pltpu.VMEM)
        hbm = pl.BlockSpec(memory_space=pl.ANY)
        res = pl.pallas_call(
            functools.partial(kernel, dims),
            out_shape=pltpu.VMEM((1, rows + wide), jnp.float32),
            in_specs=[hbm] * 6,
            out_specs=vm,
            scratch_shapes=[
                pltpu.VMEM((dp * rows, depth), jnp.bfloat16),
                pltpu.VMEM((rows, depth), jnp.bfloat16),
                pltpu.VMEM((far, share, depth), jnp.bfloat16),
                pltpu.VMEM((WSLOTS, depth, tile), jnp.bfloat16),
                pltpu.VMEM((2, 2 * rows, tile), jnp.float32),
                pltpu.VMEM((RING, rows, tile), jnp.float32),
                pltpu.VMEM((chips - 1, tiles, rows, tile), jnp.int16),
                pltpu.VMEM((chips - 1, tiles, rows, tile), jnp.int16),
                pltpu.VMEM((chips - 1, pieces, 1, rows), jnp.float32),
                pltpu.VMEM((chips - 1, pieces, 1, rows), jnp.float32),
                pltpu.VMEM(((chips - 1) * rows, LANES), jnp.float32),
                pltpu.VMEM((1, rows), jnp.int32),
                pltpu.VMEM((rows, LANES), jnp.int32),
                pltpu.VMEM((rows, LANES), jnp.float32),
                pltpu.VMEM((rows, LANES), jnp.float32),
                pltpu.VMEM((rows, LANES), jnp.float32),
                pltpu.VMEM((dp, 2, 1, rows), jnp.int32),
                pltpu.VMEM((1, samples), jnp.int32),
                pltpu.VMEM((samples, LANES), jnp.float32),
                pltpu.VMEM((2, rows), jnp.float32),
                pltpu.VMEM((dp * nv, 2, rows), jnp.float32),
                sem((WSLOTS,)), sem((len(heads),)), sem((5,)), sem((2,)), sem((far,)), sem((far,)),
                sem((far,)), sem((chips - 1,)), sem((2,)), sem((2,)),
                sem((2,)), sem((RING,)), sem((len(heads),)),
                sem, sem((chips - 1, pieces)), sem, sem((chips - 1, pieces)),
                sem((2,)), pltpu.SemaphoreType.REGULAR((max(rounds, 1),)),
            ],
            compiler_params=pltpu.CompilerParams(
                collective_id=0, has_side_effects=True, vmem_limit_bytes=62 * 1024 * 1024),
        )(hidden, out_weight, targets[None, :], segment[None, :], loss_mask[None, :],
          outside_count[None, :])
        loss, sample = pl.pallas_call(
            split,
            out_shape=(jax.ShapeDtypeStruct((1, rows), jnp.float32),
                       jax.ShapeDtypeStruct((1, samples), jnp.float32)),
            in_specs=[vm],
            out_specs=(vm, vm),
            compiler_params=pltpu.CompilerParams(vmem_limit_bytes=1024 * 1024),
        )(res)
        return loss[0], sample[0]

    return jax.shard_map(
        body,
        mesh=mesh,
        in_specs=(P("dp", None), P("dp", "vocab"), P("dp"), P("dp"), P("dp"), P()),
        out_specs=(P("dp"), P()),
        check_vma=False,
    )
```

```python
import functools

import jax
import jax.numpy as jnp
from jax import lax
from jax.experimental import pallas as pl
from jax.experimental.pallas import tpu as pltpu
from jax.sharding import PartitionSpec as P

LANES = 128
TOP = 32767.0
TINY = 1e-30
RING = 4
WSLOTS = 4
WIDTH = 512
HEAD = 128


def largest_tile(columns, most):
    tile = most
    while columns % tile:
        tile //= 2
    return tile


def kernel(dims, hidden, weight, targets, segment, mask, outside, out,
           hx, hp, cx, wbuf, ybuf, prt, qs, qr, ss, sr, scale_buf, tg, tcol, m_buf, s_buf, p_buf,
           info, outv, denom, stat, statr, wsem, wfirst, lsem, hsem, csem_s, csem_r, fsem_s, fsem_r,
           tsem, isem, ysem, prsem, prfirst, qssem, qrsem, sssem, srsem, stsem, dsem):
    dp, nv, rows, depth, tiles, tile, chunks, rounds, heads, groups = dims
    chips = dp // 2
    me, v = lax.axis_index("dp"), lax.axis_index("vocab")
    x, c = me // 2, me % 2
    partner = 2 * x + (1 - c)
    owner = 2 * lax.rem(x + 1, chips) + c
    source = 2 * lax.rem(x + chips - 1, chips) + c
    share = rows // chunks
    total_steps = chips * tiles
    extra = len(heads) - 1

    def remote(src, dst, send, recv, d, w):
        return pltpu.make_async_remote_copy(
            src_ref=src, dst_ref=dst, send_sem=send, recv_sem=recv,
            device_id=(d, w), device_id_type=pl.DeviceIdType.MESH)

    def wcopy(t, slot):
        return pltpu.make_async_copy(
            weight.at[:, pl.ds(pl.multiple_of(t * tile, tile), tile)], wbuf.at[slot], wsem.at[slot])

    def features(d):
        return pl.ds(pl.multiple_of(d * depth, depth), depth)

    def token_rows(d):
        return pl.ds(pl.multiple_of(d * rows, rows), rows)

    def chunk_rows(d, j):
        return pl.ds(pl.multiple_of(d * rows + j * share, share), share)

    def crossing(step, e):
        d = 2 * lax.rem(x + step, chips) + e
        return d, 2 * (step - 1) + e, chips - step - 1

    def cross_start():
        pltpu.make_async_copy(cx, cx, lsem.at[4]).wait()
        for step in range(1, chips):
            for e in range(2):
                d, i, r = crossing(step, e)
                remote(cx.at[i], hx.at[chunk_rows(me, v)], csem_s, csem_r.at[r], d, v).start()

    def if_sender(fn):
        if chunks < nv:
            pl.when(v < chunks)(fn)
        else:
            fn()

    barrier = pltpu.get_barrier_semaphore()

    def signal(sem, d, w):
        pl.semaphore_signal(sem, inc=1, device_id=(d, w), device_id_type=pl.DeviceIdType.MESH)

    for o in range(1, dp):
        signal(barrier, lax.rem(me + o, dp), v)
    pl.when(v >= 1)(lambda: signal(barrier, me, v - 1))
    pl.when(v < nv - 1)(lambda: signal(barrier, me, v + 1))

    to_stage = pltpu.make_async_copy(hidden.at[:, features(partner)], hp, lsem.at[0])
    to_stage.start()

    def cross_load():
        for step in range(1, chips):
            for e in range(2):
                d, i, r = crossing(step, e)
                src = hidden.at[pl.ds(pl.multiple_of(v * share, share), share), features(d)]
                pltpu.make_async_copy(src, cx.at[i], lsem.at[4]).start()

    if_sender(cross_load)
    own = pltpu.make_async_copy(hidden.at[:, features(me)], hx.at[token_rows(me)], lsem.at[1])
    own.start()

    def first_copy(k):
        cols = pl.ds(*heads[k])
        return pltpu.make_async_copy(weight.at[:, cols], wbuf.at[0, :, cols], wfirst.at[k])

    for k in range(len(heads)):
        first_copy(k).start()

    def sides(reach):
        return jnp.where(v >= reach, 1, 0) + jnp.where(v < nv - reach, 1, 0)

    pl.semaphore_wait(barrier, dp - 1 + sides(1))

    def tell(k):
        reach = 1 << k
        pl.when(v >= reach)(lambda: signal(dsem.at[k], me, v - reach))
        pl.when(v < nv - reach)(lambda: signal(dsem.at[k], me, v + reach))

    def hear(k):
        pl.semaphore_wait(dsem.at[k], sides(1 << k))

    to_partner = remote(hp, hx.at[token_rows(me)], hsem.at[0], hsem.at[1], partner, v)
    targets_copy = remote(targets, tg, tsem.at[0], tsem.at[1], source, v)

    to_stage.wait()
    to_partner.start()
    if_sender(cross_start)
    if rounds:
        tell(0)
    for k in range(1, min(WSLOTS, total_steps)):
        wcopy(k % tiles, k).start()

    local_info = [pltpu.make_async_copy(ref, info.at[me, k], lsem.at[2])
                  for k, ref in enumerate((segment, mask))]
    local_out = pltpu.make_async_copy(outside, outv, lsem.at[3])

    def info_copy(o, k, ref):
        return remote(ref, info.at[me, k], isem.at[0], isem.at[1], lax.rem(me + o, dp), v)

    def start_small():
        targets_copy.start()
        for o in range(1, dp):
            for k, ref in enumerate((segment, mask)):
                info_copy(o, k, ref).start()
        for copy in local_info:
            copy.start()
        local_out.start()

    def spread():
        for step in range(1, chips):
            blocks_wait(2 * share, csem_s, csem_r.at[step - 1], False)
            for e in range(2):
                d = 2 * lax.rem(x + step, chips) + e
                i = 2 * (step - 1) + e
                block = hx.at[chunk_rows(d, v)]

                def one(o, carry, block=block, step=step, i=i):
                    w = lax.rem(v + o, nv)
                    remote(block, block, fsem_s.at[i], fsem_r.at[step - 1], me, w).start()
                    return carry

                lax.fori_loop(1, nv, one, 0)

    def blocks_wait(count, sem_s, sem_r, send):
        block = hx.at[pl.ds(0, count)]
        copy = remote(block, block, sem_s, sem_r, partner, v)
        if send:
            copy.wait_send()
        else:
            copy.wait_recv()

    def spread_wait(step):
        if chunks < nv:
            pl.when(v < chunks)(lambda: blocks_wait(
                2 * (chunks - 1) * share, fsem_s.at[0], fsem_r.at[step - 1], False))
            pl.when(v >= chunks)(lambda: blocks_wait(
                2 * chunks * share, fsem_s.at[0], fsem_r.at[step - 1], False))
        else:
            blocks_wait(2 * (chunks - 1) * share, fsem_s.at[0], fsem_r.at[step - 1], False)

    def dot_rows(start, count, at, slot, yslot, first=0, width=tile):
        lhs = pl.ds(pl.multiple_of(start, count), count)
        cols = slice(first, first + width)
        ybuf[yslot, pl.ds(pl.multiple_of(at, count), count), cols] = jnp.dot(
            hx[lhs, :], wbuf[slot, :, cols], preferred_element_type=jnp.float32)

    def ycopy(i):
        half = pl.ds(pl.multiple_of((1 - c) * rows, rows), rows)
        slot, ring = lax.rem(i, 2), lax.rem(i, RING)
        return remote(ybuf.at[slot, half], prt.at[ring], ysem.at[slot], prsem.at[ring], partner, v)

    def first_ycopy(k):
        half = pl.ds(pl.multiple_of((1 - c) * rows, rows), rows)
        cols = pl.ds(*heads[k])
        return remote(ybuf.at[0, half, cols], prt.at[0, :, cols], ysem.at[0], prfirst.at[k], partner, v)

    def qcopy(s, t, k, first, width):
        d = 2 * lax.rem(x + chips - s - 1 + chips, chips) + c
        cols = pl.ds(first, width)
        g = sum(jnp.where(t >= start, 1, 0) for start, _ in groups[1:]) if len(groups) > 1 else 0
        return (remote(qs.at[s, t, :, cols], qr.at[s, t, :, cols], qssem, qrsem.at[s, g], d, v),
                remote(ss.at[s, k], sr.at[s, k], sssem, srsem.at[s, g], d, v))

    def group_wait(g):
        start, count = groups[g]
        low, high = (start + extra if start else 0), start + count + extra
        for a in range(chips - 1):
            block, scales = qr.at[a, pl.ds(start, count)], sr.at[a, pl.ds(low, high - low)]
            remote(block, block, qssem, qrsem.at[a, g], partner, v).wait_recv()
            remote(scales, scales, sssem, srsem.at[a, g], partner, v).wait_recv()

    band = min(rows, 32)

    def total(i, b, cols):
        mine = pl.ds(pl.multiple_of(c * rows + b * band, band), band)
        theirs = pl.ds(b * band, band)
        return ybuf[lax.rem(i, 2), mine, cols] + prt[lax.rem(i, RING), theirs, cols]

    def send_sums(s, t, k, first, width):
        i = s * tiles + t
        cols = slice(first, first + width)
        for b in range(rows // band):
            value = total(i, b, cols)
            top = jnp.maximum(jnp.max(jnp.abs(value), axis=1, keepdims=True), TINY)
            code = jnp.round(value * (TOP / top)).astype(jnp.int32)
            qs[s, t, b * band:(b + 1) * band, cols] = code.astype(jnp.int16)
            scale_buf[b * band:(b + 1) * band, :] = jnp.broadcast_to(top * (1.0 / TOP), (band, LANES))
        data, scales = qcopy(s, t, k, first, width)
        data.start()
        ss[s, k] = jnp.transpose(scale_buf[0:rows, :])[0:1, :]
        scales.start()

    def finish(s, t, k, first, width):
        i = s * tiles + t
        for a in range(chips - 1):
            scale_buf[a * rows:(a + 1) * rows, :] = jnp.transpose(
                jnp.broadcast_to(sr[a, k], (LANES, rows)))
        base = v * (tiles * tile) + t * tile + first
        lane = lax.broadcasted_iota(jnp.int32, (band, LANES), 1)
        for b in range(rows // band):
            here = slice(b * band, (b + 1) * band)
            value = total(i, b, slice(first, first + width))
            parts = []
            for j in range(width // LANES):
                part = value[:, j * LANES:(j + 1) * LANES]
                from_here = slice(first + j * LANES, first + (j + 1) * LANES)
                for a in range(chips - 1):
                    code = qr[a, t, here, from_here].astype(jnp.int32)
                    part = part + code.astype(jnp.float32) * scale_buf[a * rows + b * band:a * rows + (b + 1) * band, :]
                parts.append(part)
            old = m_buf[here, :]
            new = functools.reduce(jnp.maximum, parts, old)
            acc = s_buf[here, :] * jnp.exp(old - new)
            picked = p_buf[here, :]
            wanted = tcol[here, :] - base
            for j, part in enumerate(parts):
                acc = acc + jnp.exp(part - new)
                picked = picked + jnp.where(lane + j * LANES == wanted, part, 0.0)
            m_buf[here, :] = new
            s_buf[here, :] = acc
            p_buf[here, :] = picked

    m_buf[...] = jnp.full(m_buf.shape, -jnp.inf, jnp.float32)
    s_buf[...] = jnp.zeros(s_buf.shape, jnp.float32)
    p_buf[...] = jnp.zeros(p_buf.shape, jnp.float32)
    own.wait()

    events = []
    events.append((1, start_small))
    for k in range(rounds):
        def turn(k=k):
            hear(k)
            if k + 1 < rounds:
                tell(k + 1)
        events.append((2 + 2 * k, turn))
    events.append((2 + 2 * rounds, lambda: if_sender(spread)))

    samples = outside.shape[1]

    def prepare():
        targets_copy.wait_recv()
        tcol[...] = jnp.transpose(jnp.broadcast_to(tg[...], (LANES, rows)))
        most = info.at[pl.ds(0, dp - 1)]
        remote(most, most, isem.at[0], isem.at[1], partner, v).wait_recv()
        pltpu.make_async_copy(info.at[me], info.at[me], lsem.at[2]).wait()
        local_out.wait()
        count = jnp.zeros((samples, 1), jnp.float32)
        for d in range(dp):
            member = lax.broadcasted_iota(jnp.int32, (samples, rows), 0) == info[d, 0]
            weights = info[d, 1].astype(jnp.float32)
            count = count + jnp.sum(jnp.where(member, weights, 0.0), axis=1, keepdims=True)
        square = (lax.broadcasted_iota(jnp.int32, (samples, samples), 0)
                  == lax.broadcasted_iota(jnp.int32, (samples, samples), 1))
        away = jnp.sum(jnp.where(square, outv[...].astype(jnp.float32), 0.0), axis=1, keepdims=True)
        denom[...] = jnp.broadcast_to(jnp.maximum(count + away, 1.0), (samples, LANES))

    for s in range(chips):
        group = lax.rem(x + chips - s, chips)
        last = s == chips - 1
        if s > 0:
            spread_wait(chips - s)
        if last:
            prepare()
        piece = finish if last else send_sums

        def handle(t, s=s, piece=piece, last=last):
            ycopy(s * tiles + t).wait_recv()
            if last:
                for g, (start, _) in enumerate(groups):
                    if start > 0:
                        pl.when(t == start)(functools.partial(group_wait, g))
            piece(s, t, t + extra, 0, tile)

        def begin(i):
            slot = lax.rem(i, WSLOTS)
            wcopy(lax.rem(i, tiles), slot).wait()

            @pl.when(i + WSLOTS - 1 < total_steps)
            def _():
                wcopy(lax.rem(i + WSLOTS - 1, tiles), lax.rem(i + WSLOTS - 1, WSLOTS)).start()

            return slot

        def step(t, carry, s=s, group=group, handle=handle, begin=begin):
            i = s * tiles + t
            slot = begin(i)

            @pl.when(i >= 2)
            def _():
                ycopy(i).wait_send()

            dot_rows(group * 2 * rows, 2 * rows, 0, slot, lax.rem(i, 2))
            ycopy(i).start()

            @pl.when(t >= 2)
            def _():
                handle(t - 1)

            if s == 0:
                for at, event in events:
                    pl.when(t == min(at, tiles - 1))(event)
            return carry

        if s == 0:
            for k in range(len(heads)):
                first_copy(k).wait()
                dot_rows(me * rows, rows, c * rows, 0, 0, *heads[k])
            to_partner.wait_recv()
            for k in range(len(heads)):
                dot_rows(partner * rows, rows, (1 - c) * rows, 0, 0, *heads[k])
                first_ycopy(k).start()
            if last:
                group_wait(0)
            for k in range(len(heads)):
                first_ycopy(k).wait_recv()
                piece(s, 0, k, *heads[k])
            if tiles == 1:
                for at, event in events:
                    event()
        else:
            i = s * tiles
            slot = begin(i)
            if i >= 2:
                ycopy(i).wait_send()
            dot_rows(group * 2 * rows, 2 * rows, 0, slot, i % 2)
            ycopy(i).start()
            ycopy(i).wait_recv()
            if last:
                group_wait(0)
            for k in range(len(heads)):
                piece(s, 0, k, *heads[k])
        if tiles > 1:
            lax.fori_loop(1, tiles, step, 0)
            handle(tiles - 1)

    lane = lax.broadcasted_iota(jnp.int32, (rows, LANES), 1)
    peak = jnp.max(m_buf[...], axis=1, keepdims=True)
    mass = jnp.sum(s_buf[...] * jnp.exp(m_buf[...] - peak), axis=1, keepdims=True)
    hit = jnp.sum(p_buf[...], axis=1, keepdims=True)
    table = jnp.transpose(jnp.where(lane == 0, peak, jnp.where(lane == 1, mass, hit)))
    stat[0:1, :] = table[0:1, :] + jnp.log(table[1:2, :])
    stat[1:2, :] = table[2:3, :]

    def stat_copy(d, w):
        return remote(stat, statr.at[owner * nv + v], stsem.at[0], stsem.at[1], d, w)

    def stat_start(o, carry):
        w = lax.rem(v + o, nv)
        for k in range(dp):
            stat_copy(lax.rem(me + k, dp), w).start()
        return carry

    lax.fori_loop(1, nv, stat_start, 0)
    for k in range(1, dp):
        stat_copy(lax.rem(me + k, dp), v).start()
    statr[owner * nv + v] = stat[...]
    most = statr.at[pl.ds(0, dp * nv - 1)]
    remote(most, most, stsem.at[0], stsem.at[1], partner, v).wait_recv()

    mine = jnp.zeros((1, rows), jnp.float32)
    sums = jnp.zeros((samples, rows), jnp.float32)
    for d in range(dp):
        block = statr[d * nv:(d + 1) * nv]
        peak = jnp.max(block, axis=0)
        mass = jnp.sum(jnp.exp(block - peak[None]), axis=0)
        hit = jnp.sum(block, axis=0)
        loss = peak[0:1, :] + jnp.log(mass[0:1, :]) - hit[1:2, :]
        mine = jnp.where(me == d, loss, mine)
        member = lax.broadcasted_iota(jnp.int32, (samples, rows), 0) == info[d, 0]
        sums = sums + jnp.where(member, loss * info[d, 1].astype(jnp.float32), 0.0)
    ratio = jnp.sum(sums, axis=1, keepdims=True) / denom[:, 0:1]
    wide = out.shape[1] - rows
    diagonal = (lax.broadcasted_iota(jnp.int32, (samples, wide), 0)
                == lax.broadcasted_iota(jnp.int32, (samples, wide), 1))
    out[0:1, 0:rows] = mine
    out[0:1, rows:rows + wide] = jnp.sum(jnp.where(diagonal, ratio, 0.0), axis=0, keepdims=True)

    to_partner.wait_send()
    targets_copy.wait_send()
    most_info = info.at[pl.ds(0, dp - 1)]
    remote(most_info, most_info, isem.at[0], isem.at[1], partner, v).wait_send()

    def leave():
        remote(cx, cx, csem_s, csem_r.at[0], partner, v).wait_send()
        for step in range(1, chips):
            for e in range(2):
                i = 2 * (step - 1) + e
                blocks_wait((nv - 1) * share, fsem_s.at[i], fsem_r.at[step - 1], True)

    if_sender(leave)
    for k in range(min(2, total_steps)):
        ycopy(k).wait_send()
    remote(qs, qr, qssem, qrsem.at[0, 0], partner, v).wait_send()
    remote(ss, sr, sssem, srsem.at[0, 0], partner, v).wait_send()
    remote(most, most, stsem.at[0], stsem.at[1], partner, v).wait_send()


def split(res, loss, sample):
    rows, samples = loss.shape[1], sample.shape[1]
    loss[...] = res[:, 0:rows]
    sample[...] = res[:, rows:rows + samples]


def solution(mesh):
    dp, nv = mesh.shape["dp"], mesh.shape["vocab"]

    def body(hidden, out_weight, targets, segment, loss_mask, outside_count):
        rows = hidden.shape[0]
        depth, columns = out_weight.shape
        samples = outside_count.shape[0]
        chips = dp // 2
        tile = largest_tile(columns, WIDTH)
        tiles = columns // tile
        chunks = min(nv, rows // 16)
        share = rows // chunks
        rounds = (nv - 2).bit_length()
        heads, at = [], 0
        while at < tile:
            width = HEAD if at < 2 * HEAD and tile > HEAD else tile - at
            heads.append((at, width))
            at += width
        pieces = tiles + len(heads) - 1
        groups, left, count = [], tiles, 1
        while left:
            count = min(count, left) if left > 2 * count or left <= count else left
            groups.append((left - count, count))
            left, count = left - count, count + 1
        groups.reverse()
        dims = (dp, nv, rows, depth, tiles, tile, chunks, rounds, tuple(heads), tuple(groups))
        sem = pltpu.SemaphoreType.DMA
        far = 2 * (chips - 1)
        wide = -(-samples // LANES) * LANES
        vm = pl.BlockSpec(memory_space=pltpu.VMEM)
        hbm = pl.BlockSpec(memory_space=pl.ANY)
        res = pl.pallas_call(
            functools.partial(kernel, dims),
            out_shape=pltpu.VMEM((1, rows + wide), jnp.float32),
            in_specs=[hbm] * 6,
            out_specs=vm,
            scratch_shapes=[
                pltpu.VMEM((dp * rows, depth), jnp.bfloat16),
                pltpu.VMEM((rows, depth), jnp.bfloat16),
                pltpu.VMEM((far, share, depth), jnp.bfloat16),
                pltpu.VMEM((WSLOTS, depth, tile), jnp.bfloat16),
                pltpu.VMEM((2, 2 * rows, tile), jnp.float32),
                pltpu.VMEM((RING, rows, tile), jnp.float32),
                pltpu.VMEM((chips - 1, tiles, rows, tile), jnp.int16),
                pltpu.VMEM((chips - 1, tiles, rows, tile), jnp.int16),
                pltpu.VMEM((chips - 1, pieces, 1, rows), jnp.float32),
                pltpu.VMEM((chips - 1, pieces, 1, rows), jnp.float32),
                pltpu.VMEM(((chips - 1) * rows, LANES), jnp.float32),
                pltpu.VMEM((1, rows), jnp.int32),
                pltpu.VMEM((rows, LANES), jnp.int32),
                pltpu.VMEM((rows, LANES), jnp.float32),
                pltpu.VMEM((rows, LANES), jnp.float32),
                pltpu.VMEM((rows, LANES), jnp.float32),
                pltpu.VMEM((dp, 2, 1, rows), jnp.int32),
                pltpu.VMEM((1, samples), jnp.int32),
                pltpu.VMEM((samples, LANES), jnp.float32),
                pltpu.VMEM((2, rows), jnp.float32),
                pltpu.VMEM((dp * nv, 2, rows), jnp.float32),
                sem((WSLOTS,)), sem((len(heads),)), sem((5,)), sem((2,)), sem, sem((chips - 1,)),
                sem((far,)), sem((chips - 1,)), sem((2,)), sem((2,)),
                sem((2,)), sem((RING,)), sem((len(heads),)),
                sem, sem((chips - 1, len(groups))), sem, sem((chips - 1, len(groups))),
                sem((2,)), pltpu.SemaphoreType.REGULAR((max(rounds, 1),)),
            ],
            compiler_params=pltpu.CompilerParams(
                collective_id=0, has_side_effects=True, vmem_limit_bytes=62 * 1024 * 1024),
        )(hidden, out_weight, targets[None, :], segment[None, :], loss_mask[None, :],
          outside_count[None, :])
        loss, sample = pl.pallas_call(
            split,
            out_shape=(jax.ShapeDtypeStruct((1, rows), jnp.float32),
                       jax.ShapeDtypeStruct((1, samples), jnp.float32)),
            in_specs=[vm],
            out_specs=(vm, vm),
            compiler_params=pltpu.CompilerParams(vmem_limit_bytes=1024 * 1024),
        )(res)
        return loss[0], sample[0]

    return jax.shard_map(
        body,
        mesh=mesh,
        in_specs=(P("dp", None), P("dp", "vocab"), P("dp"), P("dp"), P("dp"), P()),
        out_specs=(P("dp"), P()),
        check_vma=False,
    )
```

```python
import functools

import jax
import jax.numpy as jnp
from jax import lax
from jax.experimental import pallas as pl
from jax.experimental.pallas import tpu as pltpu
from jax.sharding import PartitionSpec as P

LANES = 128
TOP = 32767.0
TINY = 1e-30
RING = 4
WSLOTS = 4
WIDTH = 512
HEAD = 128


def largest_tile(columns, most):
    tile = most
    while columns % tile:
        tile //= 2
    return tile


def kernel(dims, hidden, weight, targets, segment, mask, outside, out,
           hx, hp, cx, wbuf, ybuf, prt, qs, qr, ss, sr, scale_buf, tg, tcol, m_buf, s_buf, p_buf,
           info, outv, denom, stat, statr, wsem, wfirst, lsem, hsem, csem_s, csem_r, fsem_s, fsem_r,
           tsem, isem, ysem, prsem, prfirst, qssem, qrsem, sssem, srsem, stsem, dsem):
    dp, nv, rows, depth, tiles, tile, chunks, rounds, heads, groups = dims
    chips = dp // 2
    me, v = lax.axis_index("dp"), lax.axis_index("vocab")
    x, c = me // 2, me % 2
    partner = 2 * x + (1 - c)
    owner = 2 * lax.rem(x + 1, chips) + c
    source = 2 * lax.rem(x + chips - 1, chips) + c
    share = rows // chunks
    total_steps = chips * tiles
    extra = len(heads) - 1

    def remote(src, dst, send, recv, d, w):
        return pltpu.make_async_remote_copy(
            src_ref=src, dst_ref=dst, send_sem=send, recv_sem=recv,
            device_id=(d, w), device_id_type=pl.DeviceIdType.MESH)

    def wcopy(t, slot):
        return pltpu.make_async_copy(
            weight.at[:, pl.ds(pl.multiple_of(t * tile, tile), tile)], wbuf.at[slot], wsem.at[slot])

    def features(d):
        return pl.ds(pl.multiple_of(d * depth, depth), depth)

    def token_rows(d):
        return pl.ds(pl.multiple_of(d * rows, rows), rows)

    def chunk_rows(d, j):
        return pl.ds(pl.multiple_of(d * rows + j * share, share), share)

    def crossing(step, e):
        d = 2 * lax.rem(x + step, chips) + e
        return d, 2 * (step - 1) + e, chips - step - 1

    def cross_start():
        pltpu.make_async_copy(cx, cx, lsem.at[4]).wait()
        for step in range(1, chips):
            for e in range(2):
                d, i, r = crossing(step, e)
                remote(cx.at[i], hx.at[chunk_rows(me, v)], csem_s, csem_r.at[r], d, v).start()

    def if_sender(fn):
        if chunks < nv:
            pl.when(v < chunks)(fn)
        else:
            fn()

    barrier = pltpu.get_barrier_semaphore()

    def signal(sem, d, w):
        pl.semaphore_signal(sem, inc=1, device_id=(d, w), device_id_type=pl.DeviceIdType.MESH)

    for o in range(1, dp):
        signal(barrier, lax.rem(me + o, dp), v)
    pl.when(v >= 1)(lambda: signal(barrier, me, v - 1))
    pl.when(v < nv - 1)(lambda: signal(barrier, me, v + 1))

    to_stage = pltpu.make_async_copy(hidden.at[:, features(partner)], hp, lsem.at[0])

    def cross_load():
        for step in range(1, chips):
            for e in range(2):
                d, i, r = crossing(step, e)
                src = hidden.at[pl.ds(pl.multiple_of(v * share, share), share), features(d)]
                pltpu.make_async_copy(src, cx.at[i], lsem.at[4]).start()

    if_sender(cross_load)
    to_stage.start()
    own = pltpu.make_async_copy(hidden.at[:, features(me)], hx.at[token_rows(me)], lsem.at[1])
    own.start()

    def first_copy(k):
        cols = pl.ds(*heads[k])
        return pltpu.make_async_copy(weight.at[:, cols], wbuf.at[0, :, cols], wfirst.at[k])

    for k in range(len(heads)):
        first_copy(k).start()

    def sides(reach):
        return jnp.where(v >= reach, 1, 0) + jnp.where(v < nv - reach, 1, 0)

    pl.semaphore_wait(barrier, dp - 1 + sides(1))

    def tell(k):
        reach = 1 << k
        pl.when(v >= reach)(lambda: signal(dsem.at[k], me, v - reach))
        pl.when(v < nv - reach)(lambda: signal(dsem.at[k], me, v + reach))

    def hear(k):
        pl.semaphore_wait(dsem.at[k], sides(1 << k))

    to_partner = remote(hp, hx.at[token_rows(me)], hsem.at[0], hsem.at[1], partner, v)
    targets_copy = remote(targets, tg, tsem.at[0], tsem.at[1], source, v)

    if_sender(cross_start)
    to_stage.wait()
    to_partner.start()
    if rounds:
        tell(0)
    for k in range(1, min(WSLOTS, total_steps)):
        wcopy(k % tiles, k).start()

    local_info = [pltpu.make_async_copy(ref, info.at[me, k], lsem.at[2])
                  for k, ref in enumerate((segment, mask))]
    local_out = pltpu.make_async_copy(outside, outv, lsem.at[3])

    def info_copy(o, k, ref):
        return remote(ref, info.at[me, k], isem.at[0], isem.at[1], lax.rem(me + o, dp), v)

    def start_small():
        targets_copy.start()
        for o in range(1, dp):
            for k, ref in enumerate((segment, mask)):
                info_copy(o, k, ref).start()
        for copy in local_info:
            copy.start()
        local_out.start()

    def spread():
        for step in range(1, chips):
            blocks_wait(2 * share, csem_s, csem_r.at[step - 1], False)
            for e in range(2):
                d = 2 * lax.rem(x + step, chips) + e
                i = 2 * (step - 1) + e
                block = hx.at[chunk_rows(d, v)]

                def one(o, carry, block=block, step=step, i=i):
                    w = lax.rem(v + o, nv)
                    remote(block, block, fsem_s.at[i], fsem_r.at[step - 1], me, w).start()
                    return carry

                lax.fori_loop(1, nv, one, 0)

    def blocks_wait(count, sem_s, sem_r, send):
        block = hx.at[pl.ds(0, count)]
        copy = remote(block, block, sem_s, sem_r, partner, v)
        if send:
            copy.wait_send()
        else:
            copy.wait_recv()

    def spread_wait(step):
        if chunks < nv:
            pl.when(v < chunks)(lambda: blocks_wait(
                2 * (chunks - 1) * share, fsem_s.at[0], fsem_r.at[step - 1], False))
            pl.when(v >= chunks)(lambda: blocks_wait(
                2 * chunks * share, fsem_s.at[0], fsem_r.at[step - 1], False))
        else:
            blocks_wait(2 * (chunks - 1) * share, fsem_s.at[0], fsem_r.at[step - 1], False)

    def dot_rows(start, count, at, slot, yslot, first=0, width=tile):
        lhs = pl.ds(pl.multiple_of(start, count), count)
        cols = slice(first, first + width)
        ybuf[yslot, pl.ds(pl.multiple_of(at, count), count), cols] = jnp.dot(
            hx[lhs, :], wbuf[slot, :, cols], preferred_element_type=jnp.float32)

    def ycopy(i):
        half = pl.ds(pl.multiple_of((1 - c) * rows, rows), rows)
        slot, ring = lax.rem(i, 2), lax.rem(i, RING)
        return remote(ybuf.at[slot, half], prt.at[ring], ysem.at[slot], prsem.at[ring], partner, v)

    def first_ycopy(k):
        half = pl.ds(pl.multiple_of((1 - c) * rows, rows), rows)
        cols = pl.ds(*heads[k])
        return remote(ybuf.at[0, half, cols], prt.at[0, :, cols], ysem.at[0], prfirst.at[k], partner, v)

    def qcopy(s, t, k, first, width):
        d = 2 * lax.rem(x + chips - s - 1 + chips, chips) + c
        cols = pl.ds(first, width)
        g = sum(jnp.where(t >= start, 1, 0) for start, _ in groups[1:]) if len(groups) > 1 else 0
        return (remote(qs.at[s, t, :, cols], qr.at[s, t, :, cols], qssem, qrsem.at[s, g], d, v),
                remote(ss.at[s, k], sr.at[s, k], sssem, srsem.at[s, g], d, v))

    def group_wait(g):
        start, count = groups[g]
        low, high = (start + extra if start else 0), start + count + extra
        for a in range(chips - 1):
            block, scales = qr.at[a, pl.ds(start, count)], sr.at[a, pl.ds(low, high - low)]
            remote(block, block, qssem, qrsem.at[a, g], partner, v).wait_recv()
            remote(scales, scales, sssem, srsem.at[a, g], partner, v).wait_recv()

    band = min(rows, 32)

    def total(i, b, cols):
        mine = pl.ds(pl.multiple_of(c * rows + b * band, band), band)
        theirs = pl.ds(b * band, band)
        return ybuf[lax.rem(i, 2), mine, cols] + prt[lax.rem(i, RING), theirs, cols]

    def send_sums(s, t, k, first, width):
        i = s * tiles + t
        cols = slice(first, first + width)
        for b in range(rows // band):
            value = total(i, b, cols)
            top = jnp.maximum(jnp.max(jnp.abs(value), axis=1, keepdims=True), TINY)
            code = jnp.round(value * (TOP / top)).astype(jnp.int32)
            qs[s, t, b * band:(b + 1) * band, cols] = code.astype(jnp.int16)
            scale_buf[b * band:(b + 1) * band, :] = jnp.broadcast_to(top * (1.0 / TOP), (band, LANES))
        data, scales = qcopy(s, t, k, first, width)
        data.start()
        ss[s, k] = jnp.transpose(scale_buf[0:rows, :])[0:1, :]
        scales.start()

    def finish(s, t, k, first, width):
        i = s * tiles + t
        for a in range(chips - 1):
            scale_buf[a * rows:(a + 1) * rows, :] = jnp.transpose(
                jnp.broadcast_to(sr[a, k], (LANES, rows)))
        base = v * (tiles * tile) + t * tile + first
        lane = lax.broadcasted_iota(jnp.int32, (band, LANES), 1)
        for b in range(rows // band):
            here = slice(b * band, (b + 1) * band)
            value = total(i, b, slice(first, first + width))
            parts = []
            for j in range(width // LANES):
                part = value[:, j * LANES:(j + 1) * LANES]
                from_here = slice(first + j * LANES, first + (j + 1) * LANES)
                for a in range(chips - 1):
                    code = qr[a, t, here, from_here].astype(jnp.int32)
                    part = part + code.astype(jnp.float32) * scale_buf[a * rows + b * band:a * rows + (b + 1) * band, :]
                parts.append(part)
            old = m_buf[here, :]
            new = functools.reduce(jnp.maximum, parts, old)
            acc = s_buf[here, :] * jnp.exp(old - new)
            picked = p_buf[here, :]
            wanted = tcol[here, :] - base
            for j, part in enumerate(parts):
                acc = acc + jnp.exp(part - new)
                picked = picked + jnp.where(lane + j * LANES == wanted, part, 0.0)
            m_buf[here, :] = new
            s_buf[here, :] = acc
            p_buf[here, :] = picked

    m_buf[...] = jnp.full(m_buf.shape, -jnp.inf, jnp.float32)
    s_buf[...] = jnp.zeros(s_buf.shape, jnp.float32)
    p_buf[...] = jnp.zeros(p_buf.shape, jnp.float32)
    own.wait()

    events = []
    events.append((1, start_small))
    for k in range(rounds):
        def turn(k=k):
            hear(k)
            if k + 1 < rounds:
                tell(k + 1)
        events.append((2 + 2 * k, turn))
    events.append((2 + 2 * rounds, lambda: if_sender(spread)))

    samples = outside.shape[1]

    def prepare():
        targets_copy.wait_recv()
        tcol[...] = jnp.transpose(jnp.broadcast_to(tg[...], (LANES, rows)))
        most = info.at[pl.ds(0, dp - 1)]
        remote(most, most, isem.at[0], isem.at[1], partner, v).wait_recv()
        pltpu.make_async_copy(info.at[me], info.at[me], lsem.at[2]).wait()
        local_out.wait()
        count = jnp.zeros((samples, 1), jnp.float32)
        for d in range(dp):
            member = lax.broadcasted_iota(jnp.int32, (samples, rows), 0) == info[d, 0]
            weights = info[d, 1].astype(jnp.float32)
            count = count + jnp.sum(jnp.where(member, weights, 0.0), axis=1, keepdims=True)
        square = (lax.broadcasted_iota(jnp.int32, (samples, samples), 0)
                  == lax.broadcasted_iota(jnp.int32, (samples, samples), 1))
        away = jnp.sum(jnp.where(square, outv[...].astype(jnp.float32), 0.0), axis=1, keepdims=True)
        denom[...] = jnp.broadcast_to(jnp.maximum(count + away, 1.0), (samples, LANES))

    for s in range(chips):
        group = lax.rem(x + chips - s, chips)
        last = s == chips - 1
        if s > 0:
            spread_wait(chips - s)
        if last:
            prepare()
        piece = finish if last else send_sums

        def handle(t, s=s, piece=piece, last=last):
            ycopy(s * tiles + t).wait_recv()
            if last:
                for g, (start, _) in enumerate(groups):
                    if start > 0:
                        pl.when(t == start)(functools.partial(group_wait, g))
            piece(s, t, t + extra, 0, tile)

        def begin(i):
            slot = lax.rem(i, WSLOTS)
            wcopy(lax.rem(i, tiles), slot).wait()

            @pl.when(i + WSLOTS - 1 < total_steps)
            def _():
                wcopy(lax.rem(i + WSLOTS - 1, tiles), lax.rem(i + WSLOTS - 1, WSLOTS)).start()

            return slot

        def step(t, carry, s=s, group=group, handle=handle, begin=begin):
            i = s * tiles + t
            slot = begin(i)

            @pl.when(i >= 2)
            def _():
                ycopy(i).wait_send()

            dot_rows(group * 2 * rows, 2 * rows, 0, slot, lax.rem(i, 2))
            ycopy(i).start()

            @pl.when(t >= 2)
            def _():
                handle(t - 1)

            if s == 0:
                for at, event in events:
                    pl.when(t == min(at, tiles - 1))(event)
            return carry

        if s == 0:
            for k in range(len(heads)):
                first_copy(k).wait()
                dot_rows(me * rows, rows, c * rows, 0, 0, *heads[k])
            to_partner.wait_recv()
            for k in range(len(heads)):
                dot_rows(partner * rows, rows, (1 - c) * rows, 0, 0, *heads[k])
                first_ycopy(k).start()
            ahead = tiles > 1 and not last
            if ahead:
                slot = begin(1)
                dot_rows(partner * rows, rows, (1 - c) * rows, slot, 1)
                ycopy(1).start()
            if last:
                group_wait(0)
            for k in range(len(heads)):
                first_ycopy(k).wait_recv()
                piece(s, 0, k, *heads[k])
            if ahead:
                dot_rows(me * rows, rows, c * rows, slot, 1)
            for at, event in events:
                if min(at, tiles - 1) <= int(ahead):
                    event()
        else:
            i = s * tiles
            slot = begin(i)
            if i >= 2:
                ycopy(i).wait_send()
            dot_rows(group * 2 * rows, 2 * rows, 0, slot, i % 2)
            ycopy(i).start()
            ycopy(i).wait_recv()
            if last:
                group_wait(0)
            for k in range(len(heads)):
                piece(s, 0, k, *heads[k])
        if tiles > 1:
            lax.fori_loop(2 if s == 0 and ahead else 1, tiles, step, 0)
            handle(tiles - 1)

    lane = lax.broadcasted_iota(jnp.int32, (rows, LANES), 1)
    peak = jnp.max(m_buf[...], axis=1, keepdims=True)
    mass = jnp.sum(s_buf[...] * jnp.exp(m_buf[...] - peak), axis=1, keepdims=True)
    hit = jnp.sum(p_buf[...], axis=1, keepdims=True)
    table = jnp.transpose(jnp.where(lane == 0, peak, jnp.where(lane == 1, mass, hit)))
    stat[0:1, :] = table[0:1, :] + jnp.log(table[1:2, :])
    stat[1:2, :] = table[2:3, :]

    def stat_copy(d, w):
        return remote(stat, statr.at[owner * nv + v], stsem.at[0], stsem.at[1], d, w)

    def stat_start(o, carry):
        w = lax.rem(v + o, nv)
        for k in range(dp):
            stat_copy(lax.rem(me + k, dp), w).start()
        return carry

    lax.fori_loop(1, nv, stat_start, 0)
    for k in range(1, dp):
        stat_copy(lax.rem(me + k, dp), v).start()
    statr[owner * nv + v] = stat[...]
    most = statr.at[pl.ds(0, dp * nv - 1)]
    remote(most, most, stsem.at[0], stsem.at[1], partner, v).wait_recv()

    mine = jnp.zeros((1, rows), jnp.float32)
    sums = jnp.zeros((samples, rows), jnp.float32)
    for d in range(dp):
        block = statr[d * nv:(d + 1) * nv]
        peak = jnp.max(block, axis=0)
        mass = jnp.sum(jnp.exp(block - peak[None]), axis=0)
        hit = jnp.sum(block, axis=0)
        loss = peak[0:1, :] + jnp.log(mass[0:1, :]) - hit[1:2, :]
        mine = jnp.where(me == d, loss, mine)
        member = lax.broadcasted_iota(jnp.int32, (samples, rows), 0) == info[d, 0]
        sums = sums + jnp.where(member, loss * info[d, 1].astype(jnp.float32), 0.0)
    ratio = jnp.sum(sums, axis=1, keepdims=True) / denom[:, 0:1]
    wide = out.shape[1] - rows
    diagonal = (lax.broadcasted_iota(jnp.int32, (samples, wide), 0)
                == lax.broadcasted_iota(jnp.int32, (samples, wide), 1))
    out[0:1, 0:rows] = mine
    out[0:1, rows:rows + wide] = jnp.sum(jnp.where(diagonal, ratio, 0.0), axis=0, keepdims=True)

    to_partner.wait_send()
    targets_copy.wait_send()
    most_info = info.at[pl.ds(0, dp - 1)]
    remote(most_info, most_info, isem.at[0], isem.at[1], partner, v).wait_send()

    def leave():
        remote(cx, cx, csem_s, csem_r.at[0], partner, v).wait_send()
        for step in range(1, chips):
            for e in range(2):
                i = 2 * (step - 1) + e
                blocks_wait((nv - 1) * share, fsem_s.at[i], fsem_r.at[step - 1], True)

    if_sender(leave)
    for k in range(min(2, total_steps)):
        ycopy(k).wait_send()
    remote(qs, qr, qssem, qrsem.at[0, 0], partner, v).wait_send()
    remote(ss, sr, sssem, srsem.at[0, 0], partner, v).wait_send()
    remote(most, most, stsem.at[0], stsem.at[1], partner, v).wait_send()


def split(res, loss, sample):
    rows, samples = loss.shape[1], sample.shape[1]
    loss[...] = res[:, 0:rows]
    sample[...] = res[:, rows:rows + samples]


def solution(mesh):
    dp, nv = mesh.shape["dp"], mesh.shape["vocab"]

    def body(hidden, out_weight, targets, segment, loss_mask, outside_count):
        rows = hidden.shape[0]
        depth, columns = out_weight.shape
        samples = outside_count.shape[0]
        chips = dp // 2
        tile = largest_tile(columns, WIDTH)
        tiles = columns // tile
        chunks = min(nv, rows // 16)
        share = rows // chunks
        rounds = (nv - 2).bit_length()
        heads, at = [], 0
        while at < tile:
            width = HEAD if at < 2 * HEAD and tile > HEAD else tile - at
            heads.append((at, width))
            at += width
        pieces = tiles + len(heads) - 1
        groups, left, count = [], tiles, 1
        while left:
            count = min(count, left) if left > 2 * count or left <= count else left
            groups.append((left - count, count))
            left, count = left - count, count + 1
        groups.reverse()
        dims = (dp, nv, rows, depth, tiles, tile, chunks, rounds, tuple(heads), tuple(groups))
        sem = pltpu.SemaphoreType.DMA
        far = 2 * (chips - 1)
        wide = -(-samples // LANES) * LANES
        vm = pl.BlockSpec(memory_space=pltpu.VMEM)
        hbm = pl.BlockSpec(memory_space=pl.ANY)
        res = pl.pallas_call(
            functools.partial(kernel, dims),
            out_shape=pltpu.VMEM((1, rows + wide), jnp.float32),
            in_specs=[hbm] * 6,
            out_specs=vm,
            scratch_shapes=[
                pltpu.VMEM((dp * rows, depth), jnp.bfloat16),
                pltpu.VMEM((rows, depth), jnp.bfloat16),
                pltpu.VMEM((far, share, depth), jnp.bfloat16),
                pltpu.VMEM((WSLOTS, depth, tile), jnp.bfloat16),
                pltpu.VMEM((2, 2 * rows, tile), jnp.float32),
                pltpu.VMEM((RING, rows, tile), jnp.float32),
                pltpu.VMEM((chips - 1, tiles, rows, tile), jnp.int16),
                pltpu.VMEM((chips - 1, tiles, rows, tile), jnp.int16),
                pltpu.VMEM((chips - 1, pieces, 1, rows), jnp.float32),
                pltpu.VMEM((chips - 1, pieces, 1, rows), jnp.float32),
                pltpu.VMEM(((chips - 1) * rows, LANES), jnp.float32),
                pltpu.VMEM((1, rows), jnp.int32),
                pltpu.VMEM((rows, LANES), jnp.int32),
                pltpu.VMEM((rows, LANES), jnp.float32),
                pltpu.VMEM((rows, LANES), jnp.float32),
                pltpu.VMEM((rows, LANES), jnp.float32),
                pltpu.VMEM((dp, 2, 1, rows), jnp.int32),
                pltpu.VMEM((1, samples), jnp.int32),
                pltpu.VMEM((samples, LANES), jnp.float32),
                pltpu.VMEM((2, rows), jnp.float32),
                pltpu.VMEM((dp * nv, 2, rows), jnp.float32),
                sem((WSLOTS,)), sem((len(heads),)), sem((5,)), sem((2,)), sem, sem((chips - 1,)),
                sem((far,)), sem((chips - 1,)), sem((2,)), sem((2,)),
                sem((2,)), sem((RING,)), sem((len(heads),)),
                sem, sem((chips - 1, len(groups))), sem, sem((chips - 1, len(groups))),
                sem((2,)), pltpu.SemaphoreType.REGULAR((max(rounds, 1),)),
            ],
            compiler_params=pltpu.CompilerParams(
                collective_id=0, has_side_effects=True, vmem_limit_bytes=62 * 1024 * 1024),
        )(hidden, out_weight, targets[None, :], segment[None, :], loss_mask[None, :],
          outside_count[None, :])
        loss, sample = pl.pallas_call(
            split,
            out_shape=(jax.ShapeDtypeStruct((1, rows), jnp.float32),
                       jax.ShapeDtypeStruct((1, samples), jnp.float32)),
            in_specs=[vm],
            out_specs=(vm, vm),
            compiler_params=pltpu.CompilerParams(vmem_limit_bytes=1024 * 1024),
        )(res)
        return loss[0], sample[0]

    return jax.shard_map(
        body,
        mesh=mesh,
        in_specs=(P("dp", None), P("dp", "vocab"), P("dp"), P("dp"), P("dp"), P()),
        out_specs=(P("dp"), P()),
        check_vma=False,
    )
```
